32 devices in a mesh: left: 8 (over y, x, core), right: 4 (over z).
Axes of the slice: x: 2, y: 2, z: 4, core: 2. Of those that a mesh axis runs over, the one named last changes fastest.
Arguments:
- tracer: float32 [2, 1024, 256, 128], P(None, None, 'left', 'right'), may hold values from -6 to 6
- symbol_x: float32 [1024], replicated, may hold values from 0.3 to 3
- symbol_y: float32 [256], replicated, may hold values from 0.3 to 3
- symbol_z: float32 [128], replicated, may hold values from 0.3 to 3
Outputs:
- modes: float32 [2, 1024, 256, 128], P(None, 'left', 'right')
The draws below stay inside these ranges and needn't reach their ends.
All inputs are finite; a program needn't handle non-finite values.
Results may differ from the reference program's by a relative error of at most 0.00007.
Values sent between devices are 32-bit elements; how exact they have to be, the bound alone decides.
A program may use at most 256 MiB of HBM per device.

```python
import jax
import jax.numpy as jnp
from jax import lax

GRID_X = 1024
GRID_Y = 256
GRID_Z = 128
FIELDS = 2


def level_of(stream_key, extent, shards, least, largest):
    def one(position, parts):
        draws = jax.random.uniform(jax.random.fold_in(jax.random.fold_in(stream_key, 6), position), (parts,), jnp.float32, least / len(shards), largest / len(shards))
        return jnp.repeat(jnp.exp(draws), extent[position] // parts).reshape((-1,) + (1,) * (len(extent) - position - 1))

    gain = one(*shards[0])
    for cut in shards[1:]:
        gain = gain * one(*cut)
    return gain


def normal_values(own_key, extent, scale, reach, shards=(), dtype=jnp.bfloat16):
    loudness = level_of(own_key, extent, shards, -0.22, 0.18) if shards else 1.0
    entries = jax.random.normal(own_key, extent, jnp.float32) * scale * loudness
    return jnp.minimum(jnp.maximum(entries, -reach), reach).astype(dtype)


def setup_inputs(seed: int = 0) -> dict:
    splits = jax.random.split(jax.random.key(seed), 5)
    return {
        "tracer": normal_values(splits[0], (FIELDS, GRID_X, GRID_Y, GRID_Z), 1.0, 6.0, ((2, 8), (3, 4)), jnp.float32),
        "symbol_x": jnp.clip(jax.random.uniform(splits[1], (GRID_X,), jnp.float32, 0.3, 3.0), 0.3, 3.0),
        "symbol_y": jnp.clip(jax.random.uniform(splits[2], (GRID_Y,), jnp.float32, 0.3, 3.0), 0.3, 3.0),
        "symbol_z": jnp.clip(jax.random.uniform(splits[3], (GRID_Z,), jnp.float32, 0.3, 3.0), 0.3, 3.0),
    }


def transform_table(count):
    rank = jnp.arange(count)
    angle = 2.0 * jnp.pi / count * (rank[:, None] * rank[None, :] % count).astype(jnp.float32)
    return (jnp.cos(angle) + jnp.sin(angle)) * count ** (-0.5)

def transform_dim(values, dim):
    moved = jnp.tensordot(values, transform_table(values.shape[dim]), axes=([dim], [0]), precision=lax.Precision.HIGHEST)
    return jnp.moveaxis(moved, -1, dim)

def reference(tracer, symbol_x, symbol_y, symbol_z):
    modes = tracer
    modes = transform_dim(modes, 1)
    modes = transform_dim(modes, 2)
    modes = transform_dim(modes, 3)
    symbol = symbol_x[:, None, None] + symbol_y[None, :, None] + symbol_z[None, None, :]
    modes = modes * lax.rsqrt(symbol)
    return modes
```

```python
import functools

import jax
import jax.numpy as jnp
import numpy as np
from jax import lax
from jax.experimental import pallas as pl
from jax.experimental.pallas import tpu as pltpu
from jax.sharding import PartitionSpec as P

MESH = pl.DeviceIdType.MESH
HIGHEST = lax.Precision.HIGHEST
DEPTH = 8
BAND = 16
LANES = 128
SLOTS = 4


def transform_table(count):
    inner = 1 << ((count.bit_length() - 1) // 2)
    outer = count // inner
    column = np.arange(count)

    def angle(row):
        return 2.0 * np.pi / count * (row[:, None] * column[None, :] % count)

    low = angle(np.arange(inner))
    high = angle(np.arange(outer) * inner)
    scale = count ** (-0.5)
    cos_low = jnp.asarray(np.cos(low), jnp.float32)[None]
    sin_low = jnp.asarray(np.sin(low), jnp.float32)[None]
    plus = jnp.asarray((np.cos(high) + np.sin(high)) * scale, jnp.float32)[:, None]
    minus = jnp.asarray((np.cos(high) - np.sin(high)) * scale, jnp.float32)[:, None]
    return (cos_low * plus + sin_low * minus).reshape(count, count)


def landed(ref, sem):
    pltpu.make_async_copy(ref, ref, sem).wait()


def kernel(lefts, rights, data, hx, hy, hz, base, sym_y, out, first, second,
           dbuf, send_a, ybuf, send_b, zbuf, obuf,
           d_sem, sa_sem, ra_sem, y_sem, sb_sem, rb_sem, z_sem, o_sem):
    fields, share_y, share_z, _ = data.shape
    size_y, size_z = hy.shape[0], hz.shape[0]
    share_x = base.shape[0]
    bands = out.shape[1]
    pieces = share_z // DEPTH
    chunks = fields * pieces
    rows = share_y * DEPTH
    flat = DEPTH * BAND
    out_y = bands * BAND
    left, right = lax.axis_index("left"), lax.axis_index("right")

    def load(i):
        source = data.at[i // pieces, :, pl.ds(lax.rem(i, pieces) * DEPTH, DEPTH), :]
        return pltpu.make_async_copy(source, dbuf.at[lax.rem(i, 2)], d_sem.at[lax.rem(i, 2)])

    load(0).start()

    barrier = pltpu.get_barrier_semaphore()
    for k in range(1, lefts):
        pl.semaphore_signal(barrier, inc=1, device_id=(lax.rem(left + k, lefts), right), device_id_type=MESH)
    for k in range(1, rights):
        pl.semaphore_signal(barrier, inc=1, device_id=(left, lax.rem(right + k, rights)), device_id_type=MESH)
    pl.semaphore_wait(barrier, lefts + rights - 2)

    def copy_a(i, to):
        slot = lax.rem(i, SLOTS)
        return pltpu.make_async_remote_copy(
            src_ref=send_a.at[slot, to],
            dst_ref=first.at[i, pl.ds(left * rows, rows)],
            send_sem=sa_sem.at[slot, to],
            recv_sem=ra_sem.at[i, left],
            device_id=(to, right),
            device_id_type=MESH,
        )

    def copy_b(i, to, band):
        spot = right * share_z + lax.rem(i, pieces) * DEPTH
        return pltpu.make_async_remote_copy(
            src_ref=send_b.at[i, to, band],
            dst_ref=second.at[i // pieces, band, pl.ds(spot * BAND, flat)],
            send_sem=sb_sem.at[i, to, band],
            recv_sem=rb_sem.at[i, right, band],
            device_id=(left, to),
            device_id_type=MESH,
        )

    def sent_a(i):
        for k in range(1, lefts):
            copy_a(i, lax.rem(left + k, lefts)).wait_send()

    def x_step(i):
        load(i).wait()

        @pl.when(i + 1 < chunks)
        def _():
            load(i + 1).start()

        @pl.when(i >= SLOTS)
        def _():
            sent_a(i - SLOTS)

        slot = lax.rem(i, SLOTS)

        def tile(j, carry):
            lines = dbuf[lax.rem(i, 2)].reshape(rows, hx.shape[0])
            cols = pl.ds(pl.multiple_of(j * 2 * share_x, 2 * share_x), 2 * share_x)
            got = jnp.dot(lines, hx[:, cols], precision=HIGHEST, preferred_element_type=jnp.float32)
            send_a[slot, 2 * j] = got[:, :share_x]
            send_a[slot, 2 * j + 1] = got[:, share_x:]
            return carry

        lax.fori_loop(0, lefts // 2, tile, 0)
        for k in range(1, lefts):
            copy_a(i, lax.rem(left + k, lefts)).start()
        pltpu.make_async_copy(
            send_a.at[slot, left], first.at[i, pl.ds(left * rows, rows)], ra_sem.at[i, left]
        ).start()

    def y_step(i):
        for k in range(lefts):
            landed(first.at[i, pl.ds(k * rows, rows)], ra_sem.at[i, k])
        fetch = pltpu.make_async_copy(first.at[i], ybuf, y_sem)
        fetch.start()
        fetch.wait()
        for z in range(0, DEPTH, 2):
            pair = jnp.concatenate(
                [ybuf[pl.ds(z, size_y, stride=DEPTH), :], ybuf[pl.ds(z + 1, size_y, stride=DEPTH), :]], axis=1
            )
            got = jnp.dot(hy[...], pair, precision=HIGHEST, preferred_element_type=jnp.float32)
            for to in range(rights):
                for band in range(bands):
                    top = to * out_y + band * BAND
                    for half in range(2):
                        send_b[i, to, band, (z + half) * BAND:(z + half + 1) * BAND, :] = (
                            got[top:top + BAND, half * share_x:(half + 1) * share_x]
                        )
        for band in range(bands):
            for k in range(rights):
                to = jnp.where(right < rights // 2, rights - 1 - k, k)

                @pl.when(to != right)
                def _():
                    copy_b(i, to, band).start()

            spot = right * share_z + lax.rem(i, pieces) * DEPTH
            pltpu.make_async_copy(
                send_b.at[i, right, band],
                second.at[i // pieces, band, pl.ds(spot * BAND, flat)],
                rb_sem.at[i, right, band],
            ).start()

    def step(i, carry):
        @pl.when(i < chunks)
        def _():
            x_step(i)

        @pl.when(i >= 1)
        def _():
            y_step(i - 1)

        return carry

    lax.fori_loop(0, chunks + 1, step, 0)

    def put(n):
        slot = lax.rem(n, 2)
        return pltpu.make_async_copy(obuf.at[slot], out.at[n // bands, lax.rem(n, bands)], o_sem.at[slot])

    def z_step(n, carry):
        field, band = n // bands, lax.rem(n, bands)
        slot = lax.rem(n, 2)

        def arrive(p, carry):
            for k in range(rights):
                spot = k * share_z + p * DEPTH
                landed(second.at[field, band, pl.ds(spot * BAND, flat)], rb_sem.at[field * pieces + p, k, band])
            return carry

        lax.fori_loop(0, pieces, arrive, 0)
        fetch = pltpu.make_async_copy(second.at[field, band], zbuf, z_sem)
        fetch.start()
        fetch.wait()

        @pl.when(n >= 2)
        def _():
            put(n - 2).wait()

        def line(y, carry):
            plane = zbuf[pl.ds(y, size_z, stride=BAND), :].T
            got = jnp.dot(plane, hz[...], precision=HIGHEST, preferred_element_type=jnp.float32)
            got = got * lax.rsqrt(base[...] + sym_y[band * BAND + y])
            for t in range(size_z // LANES):
                obuf[slot, t, pl.ds(y, share_x, stride=BAND), :] = got[:, t * LANES:(t + 1) * LANES]
            return carry

        lax.fori_loop(0, BAND, line, 0, unroll=2)
        put(n).start()
        return carry

    steps = fields * bands
    lax.fori_loop(0, steps, z_step, 0)

    def drain_a(i, carry):
        sent_a(i)
        return carry

    lax.fori_loop(max(chunks - SLOTS, 0), chunks, drain_a, 0)

    def drain_b(i, carry):
        for k in range(1, rights):
            for band in range(bands):
                copy_b(i, lax.rem(right + k, rights), band).wait_send()
        return carry

    lax.fori_loop(0, chunks, drain_b, 0)
    for n in range(max(steps - 2, 0), steps):
        put(n).wait()


def local(lefts, rights, tracer, symbol_x, symbol_y, symbol_z):
    fields, size_x, share_y, share_z = tracer.shape
    size_y, size_z = symbol_y.shape[0], symbol_z.shape[0]
    share_x, out_y = size_x // lefts, size_y // rights
    bands = out_y // BAND
    chunks = fields * (share_z // DEPTH)
    data = jnp.transpose(tracer, (0, 2, 3, 1))
    part_x = lax.dynamic_slice_in_dim(symbol_x, lax.axis_index("left") * share_x, share_x)
    part_y = lax.dynamic_slice_in_dim(symbol_y, lax.axis_index("right") * out_y, out_y)
    base = part_x[:, None] + symbol_z[None, :]
    f32 = jnp.float32
    any_space = pl.BlockSpec(memory_space=pl.ANY)
    vmem = pl.BlockSpec(memory_space=pltpu.VMEM)
    out, _, _ = pl.pallas_call(
        functools.partial(kernel, lefts, rights),
        name="modes",
        out_shape=[
            jax.ShapeDtypeStruct((fields, bands, size_z // LANES, share_x * BAND, LANES), f32),
            jax.ShapeDtypeStruct((chunks, size_y * DEPTH, share_x), f32),
            jax.ShapeDtypeStruct((fields, bands, size_z * BAND, share_x), f32),
        ],
        in_specs=[any_space, vmem, vmem, vmem, vmem, pl.BlockSpec(memory_space=pltpu.SMEM)],
        out_specs=[any_space] * 3,
        scratch_shapes=[
            pltpu.VMEM((2, share_y, DEPTH, size_x), f32),
            pltpu.VMEM((SLOTS, lefts, share_y * DEPTH, share_x), f32),
            pltpu.VMEM((size_y * DEPTH, share_x), f32),
            pltpu.VMEM((chunks, rights, bands, DEPTH * BAND, share_x), f32),
            pltpu.VMEM((size_z * BAND, share_x), f32),
            pltpu.VMEM((2, size_z // LANES, share_x * BAND, LANES), f32),
            pltpu.SemaphoreType.DMA((2,)),
            pltpu.SemaphoreType.DMA((SLOTS, lefts)),
            pltpu.SemaphoreType.DMA((chunks, lefts)),
            pltpu.SemaphoreType.DMA,
            pltpu.SemaphoreType.DMA((chunks, rights, bands)),
            pltpu.SemaphoreType.DMA((chunks, rights, bands)),
            pltpu.SemaphoreType.DMA,
            pltpu.SemaphoreType.DMA((2,)),
        ],
        compiler_params=pltpu.CompilerParams(
            collective_id=0, has_side_effects=True, vmem_limit_bytes=60 * 2**20
        ),
    )(data, transform_table(size_x), transform_table(size_y), transform_table(size_z), base, part_y)
    out = out.reshape(fields, bands, size_z // LANES, share_x, BAND, LANES)
    return jnp.transpose(out, (0, 3, 1, 4, 2, 5)).reshape(fields, share_x, out_y, size_z)


def solution(mesh):
    return jax.shard_map(
        functools.partial(local, mesh.shape["left"], mesh.shape["right"]),
        mesh=mesh,
        in_specs=(P(None, None, "left", "right"), P(), P(), P()),
        out_specs=P(None, "left", "right", None),
        check_vma=False,
    )
```

```python
import functools
import math

import jax
import jax.numpy as jnp
import numpy as np
from jax import lax
from jax.experimental import pallas as pl
from jax.experimental.pallas import tpu as pltpu
from jax.sharding import PartitionSpec as P

MESH = pl.DeviceIdType.MESH
NEAR_BYTES = 20 * 2**20
DEPTH = 8
BAND = 16
LANES = 128
SLOTS = 3


def transform_table(count):
    inner = 1 << ((count.bit_length() - 1) // 2)
    outer = count // inner
    column = np.arange(count)

    def angle(row):
        return 2.0 * np.pi / count * (row[:, None] * column[None, :] % count)

    low = angle(np.arange(inner))
    high = angle(np.arange(outer) * inner)
    scale = count ** (-0.5)
    cos_low = jnp.asarray(np.cos(low), jnp.float32)[None]
    sin_low = jnp.asarray(np.sin(low), jnp.float32)[None]
    plus = jnp.asarray((np.cos(high) + np.sin(high)) * scale, jnp.float32)[:, None]
    minus = jnp.asarray((np.cos(high) - np.sin(high)) * scale, jnp.float32)[:, None]
    return (cos_low * plus + sin_low * minus).reshape(count, count)


def halves_of(table):
    upper = lax.reduce_precision(table, 8, 7)
    return jnp.stack([upper.astype(jnp.bfloat16), (table - upper).astype(jnp.bfloat16)])


def small_table(count):
    rank = np.arange(count)
    angle = 2.0 * np.pi / count * (rank[:, None] * rank[None, :] % count)
    table = ((np.cos(angle) + np.sin(angle)) * count ** (-0.5)).astype(np.float32)
    upper = table.astype(jnp.bfloat16)
    return jnp.asarray(np.stack([upper, (table - upper.astype(np.float32)).astype(jnp.bfloat16)]))


def split(values):
    upper = values.astype(jnp.bfloat16)
    return upper, (values - upper.astype(jnp.float32)).astype(jnp.bfloat16)


def product(a, b):
    dot = functools.partial(jnp.dot, preferred_element_type=jnp.float32)
    return dot(a[0], b[0]) + (dot(a[0], b[1]) + dot(a[1], b[0]))


def landed(ref, sem):
    pltpu.make_async_copy(ref, ref, sem).wait()


def kernel(lefts, rights, near, data, hx, hy, hz, base, sym_y, out, *rest):
    (first, second, dbuf, lines, send_a, send_b, obuf,
     d_sem, sa_sem, ra_sem, y_sem, sb_sem, rb_sem, z_sem, o_sem, *staging) = rest
    fields, share_y, share_z, _ = data.shape
    size_y, size_z = hy.shape[1], hz.shape[1]
    share_x = base.shape[0]
    bands = out.shape[1]
    pieces = share_z // DEPTH
    chunks = fields * pieces
    rows = share_y * DEPTH
    flat = DEPTH * BAND
    out_y = bands * BAND
    left, right = lax.axis_index("left"), lax.axis_index("right")

    def load(i):
        source = data.at[i // pieces, :, pl.ds(lax.rem(i, pieces) * DEPTH, DEPTH), :]
        return pltpu.make_async_copy(source, dbuf.at[lax.rem(i, 2)], d_sem.at[lax.rem(i, 2)])

    load(0).start()

    barrier = pltpu.get_barrier_semaphore()
    for k in range(1, lefts):
        pl.semaphore_signal(barrier, inc=1, device_id=(lax.rem(left + k, lefts), right), device_id_type=MESH)
    for k in range(1, rights):
        pl.semaphore_signal(barrier, inc=1, device_id=(left, lax.rem(right + k, rights)), device_id_type=MESH)
    pl.semaphore_wait(barrier, lefts + rights - 2)

    def copy_a(i, to):
        slot = lax.rem(i, SLOTS)
        return pltpu.make_async_remote_copy(
            src_ref=send_a.at[slot, to],
            dst_ref=first.at[i, pl.ds(left * rows, rows)],
            send_sem=sa_sem.at[slot, to],
            recv_sem=ra_sem.at[i, left],
            device_id=(to, right),
            device_id_type=MESH,
        )

    def copy_b(i, to, band):
        spot = right * share_z + lax.rem(i, pieces) * DEPTH
        return pltpu.make_async_remote_copy(
            src_ref=send_b.at[i, to, band],
            dst_ref=second.at[i // pieces, band, pl.ds(spot * BAND, flat)],
            send_sem=sb_sem.at[i, to, band],
            recv_sem=rb_sem.at[i, right, band],
            device_id=(left, to),
            device_id_type=MESH,
        )

    def sent_a(i):
        for k in range(1, lefts):
            copy_a(i, lax.rem(left + k, lefts)).wait_send()

    def x_step(i):
        load(i).wait()

        @pl.when(i + 1 < chunks)
        def _():
            load(i + 1).start()

        @pl.when(i >= SLOTS)
        def _():
            sent_a(i - SLOTS)

        slot = lax.rem(i, SLOTS)
        lines[0], lines[1] = split(dbuf[lax.rem(i, 2)].reshape(rows, hx.shape[1]))

        def tile(j, carry):
            cols = pl.ds(pl.multiple_of(j * 2 * share_x, 2 * share_x), 2 * share_x)
            got = product((lines[0], lines[1]), (hx[0, :, cols], hx[1, :, cols]))
            send_a[slot, 2 * j] = got[:, :share_x]
            send_a[slot, 2 * j + 1] = got[:, share_x:]
            return carry

        lax.fori_loop(0, lefts // 2, tile, 0)
        for k in range(1, lefts):
            copy_a(i, lax.rem(left + k, lefts)).start()
        pltpu.make_async_copy(
            send_a.at[slot, left], first.at[i, pl.ds(left * rows, rows)], ra_sem.at[i, left]
        ).start()

    def y_step(i):
        for k in range(lefts):
            landed(first.at[i, pl.ds(k * rows, rows)], ra_sem.at[i, k])
        if near:
            block = first.at[i]
        else:
            block = staging[0]
            fetch = pltpu.make_async_copy(first.at[i], block, y_sem)
            fetch.start()
            fetch.wait()
        for z in range(0, DEPTH, 2):
            pair = jnp.concatenate(
                [block[pl.ds(z, size_y, stride=DEPTH), :], block[pl.ds(z + 1, size_y, stride=DEPTH), :]], axis=1
            )
            got = product((hy[0], hy[1]), split(pair))
            for to in range(rights):
                for band in range(bands):
                    top = to * out_y + band * BAND
                    for half in range(2):
                        send_b[i, to, band, (z + half) * BAND:(z + half + 1) * BAND, :] = (
                            got[top:top + BAND, half * share_x:(half + 1) * share_x]
                        )
        for band in range(bands):
            for k in range(rights):
                to = jnp.where(right < rights // 2, rights - 1 - k, k)

                @pl.when(to != right)
                def _():
                    copy_b(i, to, band).start()

            spot = right * share_z + lax.rem(i, pieces) * DEPTH
            pltpu.make_async_copy(
                send_b.at[i, right, band],
                second.at[i // pieces, band, pl.ds(spot * BAND, flat)],
                rb_sem.at[i, right, band],
            ).start()

    def step(i, carry):
        @pl.when(i < chunks)
        def _():
            x_step(i)

        @pl.when(i >= 1)
        def _():
            y_step(i - 1)

        return carry

    lax.fori_loop(0, chunks + 1, step, 0)

    def put(n):
        slot = lax.rem(n, 2)
        return pltpu.make_async_copy(obuf.at[slot], out.at[n // bands, lax.rem(n, bands)], o_sem.at[slot])

    def z_step(n, carry):
        field, band = n // bands, lax.rem(n, bands)
        slot = lax.rem(n, 2)

        def arrive(p, carry):
            for k in range(rights):
                spot = k * share_z + p * DEPTH
                landed(second.at[field, band, pl.ds(spot * BAND, flat)], rb_sem.at[field * pieces + p, k, band])
            return carry

        lax.fori_loop(0, pieces, arrive, 0)
        if near:
            block = second.at[field, band]
        else:
            block = staging[1]
            fetch = pltpu.make_async_copy(second.at[field, band], block, z_sem)
            fetch.start()
            fetch.wait()

        @pl.when(n >= 2)
        def _():
            put(n - 2).wait()

        def line(y, carry):
            plane = block[pl.ds(y, size_z, stride=BAND), :].T
            got = product(split(plane), (hz[0], hz[1]))
            got = got * lax.rsqrt(base[...] + sym_y[right * out_y + band * BAND + y])
            for t in range(size_z // LANES):
                obuf[slot, t, pl.ds(y, share_x, stride=BAND), :] = got[:, t * LANES:(t + 1) * LANES]
            return carry

        lax.fori_loop(0, BAND, line, 0, unroll=2)
        put(n).start()
        return carry

    steps = fields * bands
    lax.fori_loop(0, steps, z_step, 0)

    def drain_a(i, carry):
        sent_a(i)
        return carry

    lax.fori_loop(max(chunks - SLOTS, 0), chunks, drain_a, 0)

    def drain_b(i, carry):
        for k in range(1, rights):
            for band in range(bands):
                copy_b(i, lax.rem(right + k, rights), band).wait_send()
        return carry

    lax.fori_loop(0, chunks, drain_b, 0)
    for n in range(max(steps - 2, 0), steps):
        put(n).wait()


def local(lefts, rights, tracer, symbol_x, symbol_y, symbol_z):
    fields, size_x, share_y, share_z = tracer.shape
    size_y, size_z = symbol_y.shape[0], symbol_z.shape[0]
    share_x, out_y = size_x // lefts, size_y // rights
    bands = out_y // BAND
    chunks = fields * (share_z // DEPTH)
    data = jnp.transpose(tracer, (0, 2, 3, 1))
    part_x = lax.dynamic_slice_in_dim(symbol_x, lax.axis_index("left") * share_x, share_x)
    base = part_x[:, None] + symbol_z[None, :]
    f32 = jnp.float32
    any_space = pl.BlockSpec(memory_space=pl.ANY)
    vmem = pl.BlockSpec(memory_space=pltpu.VMEM)
    landing = [(chunks, size_y * DEPTH, share_x), (fields, bands, size_z * BAND, share_x)]
    near = 4 * sum(map(math.prod, landing)) <= NEAR_BYTES
    staging = [] if near else [
        pltpu.VMEM((size_y * DEPTH, share_x), f32), pltpu.VMEM((size_z * BAND, share_x), f32)
    ]
    results = pl.pallas_call(
        functools.partial(kernel, lefts, rights, near),
        name="modes",
        out_shape=[
            jax.ShapeDtypeStruct((fields, bands, size_z // LANES, share_x * BAND, LANES), f32),
            *([] if near else [jax.ShapeDtypeStruct(shape, f32) for shape in landing]),
        ],
        in_specs=[any_space, vmem, vmem, vmem, vmem, pl.BlockSpec(memory_space=pltpu.SMEM)],
        out_specs=[any_space] * (1 if near else 3),
        scratch_shapes=[
            *([pltpu.VMEM(shape, f32) for shape in landing] if near else []),
            pltpu.VMEM((2, share_y, DEPTH, size_x), f32),
            pltpu.VMEM((2, share_y * DEPTH, size_x), jnp.bfloat16),
            pltpu.VMEM((SLOTS, lefts, share_y * DEPTH, share_x), f32),
            pltpu.VMEM((chunks, rights, bands, DEPTH * BAND, share_x), f32),
            pltpu.VMEM((2, size_z // LANES, share_x * BAND, LANES), f32),
            pltpu.SemaphoreType.DMA((2,)),
            pltpu.SemaphoreType.DMA((SLOTS, lefts)),
            pltpu.SemaphoreType.DMA((chunks, lefts)),
            pltpu.SemaphoreType.DMA,
            pltpu.SemaphoreType.DMA((chunks, rights, bands)),
            pltpu.SemaphoreType.DMA((chunks, rights, bands)),
            pltpu.SemaphoreType.DMA,
            pltpu.SemaphoreType.DMA((2,)),
            *staging,
        ],
        compiler_params=pltpu.CompilerParams(
            collective_id=0, has_side_effects=True, vmem_limit_bytes=60 * 2**20
        ),
    )(data, halves_of(transform_table(size_x)), small_table(size_y), small_table(size_z), base, symbol_y)
    out = results[0].reshape(fields, bands, size_z // LANES, share_x, BAND, LANES)
    return jnp.transpose(out, (0, 3, 1, 4, 2, 5)).reshape(fields, share_x, out_y, size_z)


def solution(mesh):
    return jax.shard_map(
        functools.partial(local, mesh.shape["left"], mesh.shape["right"]),
        mesh=mesh,
        in_specs=(P(None, None, "left", "right"), P(), P(), P()),
        out_specs=P(None, "left", "right", None),
        check_vma=False,
    )
```
